32 devices in a mesh: fsdp: 32 (over z, y, x, core).
Axes of the slice: x: 2, y: 2, z: 4, core: 2. Of those that a mesh axis runs over, the one named last changes fastest.
Arguments:
- x_saved: bfloat16 [2, 32, 1536, 1280], P(None, 'fsdp')
- grad_out: bfloat16 [32, 1536, 1280], P('fsdp')
- x_next: bfloat16 [32, 1536, 1280], P('fsdp')
- w_up: bfloat16 [2, 1280, 5120], replicated
- w_down: bfloat16 [2, 5120, 1280], replicated
- gacc_up: float32 [2, 1280, 5120], P(None, 'fsdp')
- gacc_down: float32 [2, 5120, 1280], P(None, 'fsdp')
- master_up: float32 [2, 1280, 5120], P(None, 'fsdp')
- master_down: float32 [2, 5120, 1280], P(None, 'fsdp')
- mom1_up: float32 [2, 1280, 5120], P(None, 'fsdp')
- mom1_down: float32 [2, 5120, 1280], P(None, 'fsdp')
- mom2_up: float32 [2, 1280, 5120], P(None, 'fsdp')
- mom2_down: float32 [2, 5120, 1280], P(None, 'fsdp')
Outputs:
- output 1: bfloat16 [32, 1536, 1280], P('fsdp')
- output 2: float32 [2, 1280, 5120], P(None, 'fsdp')
- output 3: float32 [2, 5120, 1280], P(None, 'fsdp')
- output 4: float32 [2, 1280, 5120], P(None, 'fsdp')
- output 5: float32 [2, 5120, 1280], P(None, 'fsdp')
- output 6: float32 [2, 1280, 5120], P(None, 'fsdp')
- output 7: float32 [2, 5120, 1280], P(None, 'fsdp')
All inputs are finite; a program needn't handle non-finite values.
Results may differ from the reference program's by a relative error of at most 0.00841707.
Values are sent between devices in bfloat16 or wider.
A program may use at most 1 GiB of HBM per device.

```python
import math
import jax
import jax.numpy as jnp
from jax import lax

LAYERS = 2
ADAM_STEP = 3
MICRO_STEPS = 2
GROUP_DEVS = 32
GLOBAL_BATCH = 32
SEQ_LEN = 1536
D_MODEL = 1280
D_FF = 5120

DEV_BATCH = GLOBAL_BATCH // GROUP_DEVS
LEARN_RATE = 0.001
BETA_ONE = 0.9
BETA_TWO = 0.95
ADAM_EPS = 1e-8
WEIGHT_DECAY = 0.1
CLIP_NORM = 0.1 * math.sqrt(2 * LAYERS * D_MODEL * D_FF)


def setup_inputs(seed: int = 0) -> dict:
    key_list = jax.random.split(jax.random.key(seed), 13)
    up_scale = D_MODEL ** -0.5
    down_scale = D_FF ** -0.5
    tok_shape = (GLOBAL_BATCH, SEQ_LEN, D_MODEL)
    up_shape = (LAYERS, D_MODEL, D_FF)
    down_shape = (LAYERS, D_FF, D_MODEL)
    master_up = jax.random.normal(key_list[3], up_shape, jnp.float32) * up_scale
    master_down = jax.random.normal(key_list[4], down_shape, jnp.float32) * down_scale
    w_up = master_up + 0.3 * up_scale * jax.random.normal(key_list[5], up_shape, jnp.float32)
    w_down = master_down + 0.3 * down_scale * jax.random.normal(key_list[6], down_shape, jnp.float32)
    grad_scale = (GLOBAL_BATCH * SEQ_LEN) ** -0.5
    return {
        "x_saved": jax.random.normal(key_list[0], (LAYERS,) + tok_shape, jnp.float32).astype(jnp.bfloat16),
        "grad_out": (grad_scale * jax.random.normal(key_list[1], tok_shape, jnp.float32)).astype(jnp.bfloat16),
        "x_next": jax.random.normal(key_list[2], tok_shape, jnp.float32).astype(jnp.bfloat16),
        "w_up": w_up.astype(jnp.bfloat16),
        "w_down": w_down.astype(jnp.bfloat16),
        "gacc_up": 0.3 * jax.random.normal(key_list[7], up_shape, jnp.float32),
        "gacc_down": 0.6 * jax.random.normal(key_list[8], down_shape, jnp.float32),
        "master_up": master_up,
        "master_down": master_down,
        "mom1_up": 0.01 * jax.random.normal(key_list[9], up_shape, jnp.float32),
        "mom1_down": 0.01 * jax.random.normal(key_list[10], down_shape, jnp.float32),
        "mom2_up": 0.0004 * (0.5 + jax.random.uniform(key_list[11], up_shape, jnp.float32)),
        "mom2_down": 0.0004 * (0.5 + jax.random.uniform(key_list[12], down_shape, jnp.float32)),
    }


def gelu_fn(pre_act):
    return jax.nn.gelu(pre_act, approximate=True)


def seq_backward(w_up, w_down, x_layers, grad_seq):
    grads_up = []
    grads_down = []
    grad_cur = grad_seq
    for layer_idx in range(LAYERS - 1, -1, -1):
        x_in = x_layers[layer_idx]
        pre_act = jnp.dot(x_in, w_up[layer_idx], preferred_element_type=jnp.float32)
        hidden_act, gelu_vjp = jax.vjp(gelu_fn, pre_act)
        d_act = jnp.dot(grad_cur, w_down[layer_idx].T, preferred_element_type=jnp.float32)
        d_pre = gelu_vjp(d_act)[0].astype(jnp.bfloat16)
        grads_down.append(jnp.dot(hidden_act.astype(jnp.bfloat16).T, grad_cur, preferred_element_type=jnp.float32))
        grads_up.append(jnp.dot(x_in.T, d_pre, preferred_element_type=jnp.float32))
        if layer_idx > 0:
            grad_cur = (grad_cur.astype(jnp.float32) + jnp.dot(d_pre, w_up[layer_idx].T, preferred_element_type=jnp.float32)).astype(jnp.bfloat16)
    return jnp.stack(grads_up[::-1]), jnp.stack(grads_down[::-1])


def device_partials(w_up, w_down, x_dev, grad_dev):
    def scan_body(acc_in, seq_idx):
        up_grad, down_grad = seq_backward(w_up, w_down, x_dev[:, seq_idx], grad_dev[seq_idx])
        return (acc_in[0] + up_grad, acc_in[1] + down_grad), None
    start_acc = (jnp.zeros((LAYERS, D_MODEL, D_FF), jnp.float32), jnp.zeros((LAYERS, D_FF, D_MODEL), jnp.float32))
    acc_pair, _ = lax.scan(scan_body, start_acc, jnp.arange(DEV_BATCH))
    return acc_pair[0].astype(jnp.bfloat16), acc_pair[1].astype(jnp.bfloat16)


def adamw_update(master_old, mom_one, mom_two, grad_clip):
    mom_one_new = BETA_ONE * mom_one + (1.0 - BETA_ONE) * grad_clip
    mom_two_new = BETA_TWO * mom_two + (1.0 - BETA_TWO) * grad_clip * grad_clip
    first_hat = mom_one_new / (1.0 - BETA_ONE ** ADAM_STEP)
    second_hat = mom_two_new / (1.0 - BETA_TWO ** ADAM_STEP)
    master_new = master_old - LEARN_RATE * (first_hat / (jnp.sqrt(second_hat) + ADAM_EPS) + WEIGHT_DECAY * master_old)
    return master_new, mom_one_new, mom_two_new


def seq_forward(w_up_new, w_down_new, x_seq):
    hidden_state = x_seq
    for layer_idx in range(LAYERS):
        pre_act = jnp.dot(hidden_state, w_up_new[layer_idx], preferred_element_type=jnp.float32)
        hidden_act = gelu_fn(pre_act).astype(jnp.bfloat16)
        hidden_state = (hidden_state.astype(jnp.float32) + jnp.dot(hidden_act, w_down_new[layer_idx], preferred_element_type=jnp.float32)).astype(jnp.bfloat16)
    return hidden_state


def reference(x_saved, grad_out, x_next, w_up, w_down, gacc_up, gacc_down, master_up, master_down, mom1_up, mom1_down, mom2_up, mom2_down):
    x_groups = x_saved.reshape(LAYERS, GROUP_DEVS, DEV_BATCH, SEQ_LEN, D_MODEL)
    grad_groups = grad_out.reshape(GROUP_DEVS, DEV_BATCH, SEQ_LEN, D_MODEL)

    def dev_body(acc_in, dev_idx):
        part_up, part_down = device_partials(w_up, w_down, x_groups[:, dev_idx], grad_groups[dev_idx])
        return (acc_in[0] + part_up.astype(jnp.float32), acc_in[1] + part_down.astype(jnp.float32)), None

    start_acc = (jnp.zeros((LAYERS, D_MODEL, D_FF), jnp.float32), jnp.zeros((LAYERS, D_FF, D_MODEL), jnp.float32))
    acc_pair, _ = lax.scan(dev_body, start_acc, jnp.arange(GROUP_DEVS))
    grad_up = (gacc_up + acc_pair[0]) / MICRO_STEPS
    grad_down = (gacc_down + acc_pair[1]) / MICRO_STEPS
    total_norm = jnp.sqrt(jnp.sum(grad_up * grad_up) + jnp.sum(grad_down * grad_down))
    clip_factor = jnp.minimum(1.0, CLIP_NORM / total_norm)
    new_up = adamw_update(master_up, mom1_up, mom2_up, grad_up * clip_factor)
    new_down = adamw_update(master_down, mom1_down, mom2_down, grad_down * clip_factor)
    w_up_new = new_up[0].astype(jnp.bfloat16)
    w_down_new = new_down[0].astype(jnp.bfloat16)
    x_out = lax.map(lambda x_seq: seq_forward(w_up_new, w_down_new, x_seq), x_next)
    return (x_out, new_up[0], new_down[0], new_up[1], new_down[1], new_up[2], new_down[2])
```

```python
import functools
import math
import jax
import jax.numpy as jnp
from jax import lax
from jax.experimental import pallas as pl
from jax.experimental.pallas import tpu as pltpu
from jax.sharding import PartitionSpec as P


LEARN_RATE = 0.001
BETA_ONE = 0.9
BETA_TWO = 0.95
ADAM_EPS = 1e-8
WEIGHT_DECAY = 0.1
ADAM_STEP = 3
MICRO_STEPS = 2
GELU_SCALE = math.sqrt(2.0 / math.pi)
GELU_CUBIC = 0.044715


F32 = jnp.float32
BF16 = jnp.bfloat16
MASKS = {"z": 8, "y": 4, "x": 2, "c": 1}
SIZES = {"z": 4, "y": 2, "x": 2, "c": 2}


def gelu_fn(pre_act):
    return jax.nn.gelu(pre_act, approximate=True)


def adamw_update(master_old, mom_one, mom_two, grad_clip):
    mom_one_new = BETA_ONE * mom_one + (1.0 - BETA_ONE) * grad_clip
    mom_two_new = BETA_TWO * mom_two + (1.0 - BETA_TWO) * grad_clip * grad_clip
    first_hat = mom_one_new / (1.0 - BETA_ONE ** ADAM_STEP)
    second_hat = mom_two_new / (1.0 - BETA_TWO ** ADAM_STEP)
    master_new = master_old - LEARN_RATE * (first_hat / (jnp.sqrt(second_hat) + ADAM_EPS) + WEIGHT_DECAY * master_old)
    return master_new, mom_one_new, mom_two_new


def dot(lhs, rhs, lhs_dim, rhs_dim):
    return lax.dot_general(lhs, rhs, (((lhs_dim,), (rhs_dim,)), ((), ())), preferred_element_type=F32)


def pick(value, axis, index):
    return lax.dynamic_index_in_dim(value, index, axis, keepdims=False)


class Chain:
    def __init__(self):
        self.last = None
        self.index = 0

    def step(self, compute, values, wait=None):
        self.index += 1
        if self.last is not None:
            values, _ = lax.optimization_barrier((values, self.last))
        result = compute(values)
        self.last = result if wait is None else wait(result)
        return result


class Place:
    def __init__(self, n_dev, chain):
        dev = lax.axis_index("fsdp")
        self.n_dev = n_dev
        self.chain = chain
        self.at = {"c": dev & 1, "x": (dev >> 1) & 1, "y": (dev >> 2) & 1, "z": dev >> 3}

    def swap(self, value, mask):
        return lax.ppermute(value, "fsdp", [(i, i ^ mask) for i in range(self.n_dev)])


class Reduce:
    def __init__(self, place, part, rows, order, cols=None, depth=4):
        self.place, self.order = place, order
        self.dims = ["z", "y", "x"]
        self.rows, self.depth = rows, depth
        self.cols = cols or (0, part.shape[1])
        self.part = part.reshape(depth, 2, 2, 2, rows, part.shape[1])

    def block(self, part, dim, flip, flip_core):
        sizes = [self.depth, 2, 2, 1, self.rows, self.cols[1] - self.cols[0]]
        starts = [0, 0, 0, self.place.at["c"] ^ flip_core, 0, self.cols[0]]
        axis = self.dims.index(dim)
        sizes[axis] = 1
        starts[axis] = self.place.at[dim] ^ flip
        piece = lax.dynamic_slice(part, starts, sizes)
        return piece.reshape([n for i, n in enumerate(sizes) if i not in (3, axis)])

    def first(self):
        dim = self.order[0]
        flips = [(flip, core) for flip in range(SIZES[dim]) for core in (0, 1)]
        pieces = self.place.chain.step(lambda part: [self.block(part, dim, *flip) for flip in flips[1:]], self.part)
        self.terms = [self.block(self.part, dim, 0, 0)]
        for (flip, core), piece in zip(flips[1:], pieces):
            self.terms.append(self.place.swap(piece, flip * MASKS[dim] + core))
        self.dims.remove(dim)
        self.stage = 1

    def total(self, terms, axis, index):
        picked = [pick(term, axis, index).astype(F32) for term in terms]
        while len(picked) > 1:
            picked = [sum(picked[i:i + 2]) for i in range(0, len(picked), 2)]
        return picked[0]

    def next(self):
        dim = self.order[self.stage]
        axis = self.dims.index(dim)
        mine = self.place.at[dim]
        flips = range(1, SIZES[dim])
        sends = self.place.chain.step(lambda terms: [self.total(terms, axis, mine ^ flip) for flip in flips], self.terms)
        self.terms = [pick(term, axis, mine) for term in self.terms]
        self.terms += [self.place.swap(send, flip * MASKS[dim]) for flip, send in zip(flips, sends)]
        self.dims.remove(dim)
        self.stage += 1

    def sum(self, terms):
        return self.total([term[None] for term in terms], 0, 0)


class ReduceSplit:
    def __init__(self, place, low, high):
        self.place, self.low, self.high = place, low, high

    def merge(self):
        def both(terms):
            whole = jnp.concatenate([self.low.sum(terms[0]), self.high.sum(terms[1])], axis=0)
            return [pick(whole, 0, self.place.at["z"] ^ flip) for flip in range(4)]

        sends = self.place.chain.step(both, (self.low.terms, self.high.terms))
        self.terms = [sends[0]] + [self.place.swap(sends[flip], 8 * flip) for flip in (1, 2, 3)]

    def sum(self, terms):
        return sum(terms)


def join_kernel(last, where, own, far, own_core, far_core, *refs):
    out = refs[-1]
    core = where[3]
    bit = where[{"y": 1, "x": 2}[last]]
    for ref, flip, flip_core in ((own, 0, 0), (far, 1, 0), (own_core, 0, 1), (far_core, 1, 1)):
        if last == "x":
            out[0, 0, bit ^ flip, core ^ flip_core] = ref[0, 0]
        else:
            out[0, bit ^ flip, 0, core ^ flip_core] = ref[0, 0]


def join(last, where, pieces, whole, cols, half):
    rows, part = pieces[0].shape[2:]

    def in_map(i, j, where):
        return (i, j, 0, 0)

    def out_map(i, j, where):
        if last == "x":
            return (where[0] ^ j, where[1] ^ i, 0, 0, 0, half)
        return (where[0] ^ j, 0, where[2] ^ i, 0, 0, half)

    block = (1, 1, 2, 2, rows, part) if last == "x" else (1, 2, 1, 2, rows, part)
    in_specs = [pl.BlockSpec((1, 1, rows, part), in_map)] * 4
    args = list(pieces)
    aliases = {}
    if whole is not None:
        in_specs = in_specs + [pl.BlockSpec(memory_space=pl.ANY)]
        args.append(whole)
        aliases = {5: 0}
    return pl.pallas_call(
        functools.partial(join_kernel, last),
        grid_spec=pltpu.PrefetchScalarGridSpec(num_scalar_prefetch=1, grid=(2, 4), in_specs=in_specs, out_specs=pl.BlockSpec(block, out_map)),
        out_shape=jax.ShapeDtypeStruct((4, 2, 2, 2, rows, cols), BF16),
        input_output_aliases=aliases,
        cost_estimate=pl.CostEstimate(flops=10 ** 9, bytes_accessed=8 * 8 * rows * part * 2, transcendentals=0),
    )(where, *args)


class Gather:
    def __init__(self, place, where, shard):
        self.place, self.where, self.cols = place, where, shard.shape[1]
        self.shard = shard
        self.second = ["y", "x"]
        self.third = ["x", "y"]

    def send_z(self):
        half = self.cols // 2
        pieces = self.place.chain.step(lambda shard: [shard[:, :half], shard[:, half:]], self.shard)
        self.pieces = [[piece] + [self.place.swap(piece, 8 * flip) for flip in (1, 2, 3)] for piece in pieces]

    def send_second(self):
        stacks = self.place.chain.step(lambda pieces: [jnp.stack(piece) for piece in pieces], self.pieces)
        self.pieces = [[stack, self.place.swap(stack, MASKS[dim])] for stack, dim in zip(stacks, self.second)]

    def send_third(self):
        stacks = self.place.chain.step(lambda pieces: [jnp.stack(piece) for piece in pieces], self.pieces)
        self.pieces = [[stack, self.place.swap(stack, MASKS[dim]), self.place.swap(stack, 1)] for stack, dim in zip(stacks, self.third)]

    def send_core(self):
        far = self.place.chain.step(lambda value: value, [piece[1] for piece in self.pieces])
        self.pieces = [[piece[0], got, piece[2], self.place.swap(got, 1)] for piece, got in zip(self.pieces, far)]

    def whole(self):
        def both(pieces):
            left = join("x", self.where, pieces[0], None, self.cols, 0)
            return join("y", self.where, pieces[1], left, self.cols, 1).reshape(-1, self.cols)

        return self.place.chain.step(both, self.pieces)


def hidden_kernel(n_split, x_ref, g_ref, up_ref, down_ref, *refs):
    act_ref, pre_ref = refs[-2:]
    step = x_ref.shape[0] // n_split
    for i in range(n_split):
        rows = pl.ds(i * step, step)
        h = dot(x_ref[rows, :], up_ref[...], 1, 0)
        d_act = dot(g_ref[rows, :], down_ref[...], 1, 1)
        square = h * h
        t = jnp.tanh(GELU_SCALE * h * (1.0 + GELU_CUBIC * square))
        half = 0.5 * (1.0 + t)
        slope = half + 0.5 * h * (1.0 - t * t) * (GELU_SCALE * (1.0 + 3.0 * GELU_CUBIC * square))
        act_ref[rows, :] = (h * half).astype(BF16)
        pre_ref[rows, :] = (d_act * slope).astype(BF16)


def hidden_pair(layer, x_tokens, grad_cur, w_up, w_down, part=0, n_parts=1, slopes=None):
    _, tokens, width = x_tokens.shape
    ff_width = w_up.shape[2]
    tile = 512
    steps = ff_width // tile // n_parts
    base = part * steps
    kernel = functools.partial(hidden_kernel, 6)
    in_specs = [
        pl.BlockSpec((None, tokens, width), lambda j: (layer, 0, 0)),
        pl.BlockSpec((tokens, width), lambda j: (0, 0)),
        pl.BlockSpec((None, width, tile), lambda j: (layer, 0, base + j)),
        pl.BlockSpec((None, tile, width), lambda j: (layer, base + j, 0)),
    ]
    args = [x_tokens, grad_cur, w_up, w_down]
    aliases = {}
    if slopes is not None:
        in_specs.append(pl.BlockSpec(memory_space=pl.ANY))
        args.append(slopes)
        aliases = {4: 1}
    return pl.pallas_call(
        kernel,
        grid=(steps,),
        in_specs=in_specs,
        out_specs=[pl.BlockSpec((tokens, tile), lambda j: (0, j)), pl.BlockSpec((tokens, tile), lambda j: (0, base + j))],
        out_shape=(jax.ShapeDtypeStruct((tokens, ff_width // n_parts), BF16), jax.ShapeDtypeStruct((tokens, ff_width), BF16)),
        input_output_aliases=aliases,
        compiler_params=pltpu.CompilerParams(vmem_limit_bytes=56 * 2 ** 20),
        cost_estimate=pl.CostEstimate(flops=4 * tokens * width * ff_width // n_parts, bytes_accessed=70 * 10 ** 6 // n_parts, transcendentals=tokens * ff_width // n_parts),
    )(*args)


def total_square(value, place):
    value = value.reshape(1, 1)
    value = value + place.swap(value, 1) + place.swap(value, 2) + place.swap(value, 3)
    value = value + place.swap(value, 4) + place.swap(value, 8) + place.swap(value, 12)
    return (value + place.swap(value, 16))[0, 0]


def solution(mesh):
    n_dev = mesh.shape["fsdp"]
    rows_spec = P(None, "fsdp")

    def run(x_saved, grad_out, x_next, w_up, w_down, gacc_up, gacc_down, master_up, master_down, mom1_up, mom1_down, mom2_up, mom2_down):
        chain = Chain()
        place = Place(n_dev, chain)
        layers, model_width, ff_width = w_up.shape
        clip_norm = 0.1 * math.sqrt(2 * layers * model_width * ff_width)
        x_tokens = x_saved.reshape(layers, -1, model_width)
        grad_two = grad_out.reshape(-1, model_width)
        rows_up, rows_down = gacc_up.shape[1], gacc_down.shape[1]

        def weight_grad(pair):
            return dot(pair[0], pair[1], 0, 0).astype(BF16)

        def split(part, rows, *orders):
            cols = part.shape[1] // len(orders)
            return [Reduce(place, part, rows, order, (i * cols, (i + 1) * cols)) for i, order in enumerate(orders)]

        act_low, slopes = chain.step(lambda v: hidden_pair(1, *v, part=0, n_parts=2), (x_tokens, grad_two, w_up, w_down))
        down_low = Reduce(place, chain.step(weight_grad, (act_low, grad_two)), rows_down, "xy", depth=2)
        down_low.first()
        act_high, pre_two = chain.step(lambda v: hidden_pair(1, *v[:4], part=1, n_parts=2, slopes=v[4]), (x_tokens, grad_two, w_up, w_down, slopes))
        down_high = Reduce(place, chain.step(weight_grad, (act_high, grad_two)), rows_down, "yx", depth=2)
        down_high.first()
        down_two = ReduceSplit(place, down_low, down_high)
        up_two = split(chain.step(weight_grad, (x_tokens[1], pre_two)), rows_up, "xyz", "yxz")
        for chunk in up_two:
            chunk.first()
        grad_one = chain.step(lambda v: (v[1].astype(F32) + dot(v[0], v[2], 1, 1)).astype(BF16), (pre_two, grad_two, w_up[1]))
        down_low.next()
        act_one, pre_one = chain.step(lambda v: hidden_pair(0, *v), (x_tokens, grad_one, w_up, w_down))
        down_high.next()
        down_one = split(chain.step(weight_grad, (act_one, grad_one)), rows_down, "xyz", "yxz")
        for chunk in down_one:
            chunk.first()
        for chunk in up_two:
            chunk.next()
        up_one = split(chain.step(weight_grad, (x_tokens[0], pre_one)), rows_up, "xyz", "yxz", "xyz", "yxz")
        down_two.merge()
        up_one[0].first()
        up_one[1].first()
        for chunk in up_two:
            chunk.next()
        for chunk in down_one:
            chunk.next()
        up_one[2].first()
        up_one[3].first()
        up_one[0].next()
        up_one[1].next()
        for chunk in down_one:
            chunk.next()
        up_one[2].next()
        up_one[3].next()

        def grads_of(chunks):
            def add(values):
                terms, gacc = values
                sums = [chunk.sum(term) for chunk, term in zip(chunks, terms)]
                return (gacc + (sums[0] if len(sums) == 1 else jnp.concatenate(sums, axis=1))) / MICRO_STEPS

            return add

        def finish(chunks, gacc):
            return chain.step(grads_of(chunks), ([chunk.terms for chunk in chunks], gacc))

        up_one[0].next()
        up_one[1].next()
        grad_down_two = finish([down_two], gacc_down[1])
        grad_up_two = finish(up_two, gacc_up[1])
        grad_down_one = finish(down_one, gacc_down[0])
        up_one[2].next()
        up_one[3].next()
        grad_up_one = finish(up_one, gacc_up[0])

        grads = (grad_up_one, grad_down_one, grad_up_two, grad_down_two)
        local_sq = chain.step(lambda v: sum(jnp.sum(g * g) for g in v), grads)
        clip_factor = jnp.minimum(1.0, clip_norm / jnp.sqrt(total_square(local_sq, place)))
        chain.last = None
        new_up = chain.step(lambda v: adamw_update(*v[:3], jnp.stack(v[3:5]) * v[5]), (master_up, mom1_up, mom2_up, grad_up_one, grad_up_two, clip_factor))
        where = jnp.stack([place.at[d] for d in "zyxc"]).astype(jnp.int32)
        up_a, up_b = [Gather(place, where, new_up[0][i].astype(BF16)) for i in (0, 1)]
        up_a.send_z()
        new_down = chain.step(lambda v: adamw_update(*v[:3], jnp.stack(v[3:5]) * v[5]), (master_down, mom1_down, mom2_down, grad_down_one, grad_down_two, clip_factor))
        down_a, down_b = [Gather(place, where, new_down[0][i].astype(BF16)) for i in (0, 1)]
        down_a.send_z()
        up_b.send_z()
        up_a.send_second()
        down_b.send_z()
        up_a.send_third()
        down_a.send_second()
        up_a.send_core()
        down_a.send_third()
        up_b.send_second()

        def up_mul(values):
            return gelu_fn(dot(values[0], values[1], 1, 0)).astype(BF16)

        def down_mul(values):
            return (values[0].astype(F32) + dot(values[1], values[2], 1, 0)).astype(BF16)

        hidden_state = x_next.reshape(-1, model_width)
        act = chain.step(up_mul, (hidden_state, up_a.whole()))
        down_a.send_core()
        up_b.send_third()
        down_b.send_second()
        hidden_state = chain.step(down_mul, (hidden_state, act, down_a.whole()))
        up_b.send_core()
        down_b.send_third()
        act = chain.step(up_mul, (hidden_state, up_b.whole()))
        down_b.send_core()
        hidden_state = chain.step(down_mul, (hidden_state, act, down_b.whole()))
        return (hidden_state.reshape(x_next.shape), new_up[0], new_down[0], new_up[1], new_down[1], new_up[2], new_down[2])

    return jax.shard_map(run, mesh=mesh, in_specs=(rows_spec, P("fsdp"), P("fsdp"), P(), P(), rows_spec, rows_spec, rows_spec, rows_spec, rows_spec, rows_spec, rows_spec, rows_spec), out_specs=(P("fsdp"), rows_spec, rows_spec, rows_spec, rows_spec, rows_spec, rows_spec), check_vma=False)
```

```python
import functools
import math
import jax
import jax.numpy as jnp
from jax import lax
from jax.experimental import pallas as pl
from jax.experimental.pallas import tpu as pltpu
from jax.sharding import PartitionSpec as P


LEARN_RATE = 0.001
BETA_ONE = 0.9
BETA_TWO = 0.95
ADAM_EPS = 1e-8
WEIGHT_DECAY = 0.1
ADAM_STEP = 3
MICRO_STEPS = 2
GELU_SCALE = math.sqrt(2.0 / math.pi)
GELU_CUBIC = 0.044715


F32 = jnp.float32
BF16 = jnp.bfloat16
MASKS = {"z": 8, "y": 4, "x": 2, "c": 1}
SIZES = {"z": 4, "y": 2, "x": 2, "c": 2}


def adamw_update(master_old, mom_one, mom_two, grad_clip):
    mom_one_new = BETA_ONE * mom_one + (1.0 - BETA_ONE) * grad_clip
    mom_two_new = BETA_TWO * mom_two + (1.0 - BETA_TWO) * grad_clip * grad_clip
    first_hat = mom_one_new / (1.0 - BETA_ONE ** ADAM_STEP)
    second_hat = mom_two_new / (1.0 - BETA_TWO ** ADAM_STEP)
    master_new = master_old - LEARN_RATE * (first_hat / (jnp.sqrt(second_hat) + ADAM_EPS) + WEIGHT_DECAY * master_old)
    return master_new, mom_one_new, mom_two_new


def dot(lhs, rhs, lhs_dim, rhs_dim):
    return lax.dot_general(lhs, rhs, (((lhs_dim,), (rhs_dim,)), ((), ())), preferred_element_type=F32)


def pick(value, axis, index):
    return lax.dynamic_index_in_dim(value, index, axis, keepdims=False)


class Chain:
    def __init__(self):
        self.last = None
        self.index = 0

    def step(self, compute, values, wait=None):
        self.index += 1
        if self.last is not None:
            values, _ = lax.optimization_barrier((values, self.last))
        result = compute(values)
        self.last = result if wait is None else wait(result)
        return result


class Place:
    def __init__(self, n_dev, chain):
        dev = lax.axis_index("fsdp")
        self.n_dev = n_dev
        self.chain = chain
        self.at = {"c": dev & 1, "x": (dev >> 1) & 1, "y": (dev >> 2) & 1, "z": dev >> 3}

    def swap(self, value, mask):
        return lax.ppermute(value, "fsdp", [(i, i ^ mask) for i in range(self.n_dev)])


class Reduce:
    def __init__(self, place, part, rows, order, cols=None, depth=4):
        self.place, self.order = place, order
        self.dims = ["z", "y", "x"]
        self.rows, self.depth = rows, depth
        self.cols = (0, part.shape[1]) if cols is None else cols
        self.part = None if part is None else part.reshape(depth, 2, 2, 2, rows, part.shape[1])

    def block(self, part, dim, flip, flip_core):
        sizes = [self.depth, 2, 2, 1, self.rows, self.cols[1] - self.cols[0]]
        starts = [0, 0, 0, self.place.at["c"] ^ flip_core, 0, self.cols[0]]
        axis = self.dims.index(dim)
        sizes[axis] = 1
        starts[axis] = self.place.at[dim] ^ flip
        piece = lax.dynamic_slice(part, starts, sizes)
        return piece.reshape([n for i, n in enumerate(sizes) if i not in (3, axis)])

    def first(self):
        dim = self.order[0]
        flips = [(flip, core) for flip in range(SIZES[dim]) for core in (0, 1)]
        pieces = self.place.chain.step(lambda part: [self.block(part, dim, *flip) for flip in flips[1:]], self.part)
        self.terms = [self.block(self.part, dim, 0, 0)]
        for (flip, core), piece in zip(flips[1:], pieces):
            self.terms.append(self.place.swap(piece, flip * MASKS[dim] + core))
        self.dims.remove(dim)
        self.stage = 1

    def total(self, terms, axis, index):
        picked = [pick(term, axis, index).astype(F32) for term in terms]
        while len(picked) > 1:
            picked = [sum(picked[i:i + 2]) for i in range(0, len(picked), 2)]
        return picked[0]

    def next(self):
        dim = self.order[self.stage]
        axis = self.dims.index(dim)
        mine = self.place.at[dim]
        flips = range(1, SIZES[dim])
        sends = self.place.chain.step(lambda terms: [self.total(terms, axis, mine ^ flip) for flip in range(SIZES[dim])], self.terms)
        self.terms = [sends[0]] + [self.place.swap(sends[flip], flip * MASKS[dim]) for flip in flips]
        self.dims.remove(dim)
        self.stage += 1

    def sum(self, terms):
        return self.total([term[None] for term in terms], 0, 0)


class Merge:
    def __init__(self, place, chunks, by_rows=False):
        self.place = place
        low = place.at["z"] & 1

        def near(all_terms):
            parts = [chunk.sum(terms) for chunk, terms in zip(chunks, all_terms)]
            if by_rows:
                whole = jnp.stack(parts)
            else:
                whole = jnp.concatenate(parts, axis=2)
                whole = whole.reshape(2, 2, *whole.shape[1:])
            return pick(whole, 1, low), pick(whole, 1, 1 - low)

        own, send = place.chain.step(near, [chunk.terms for chunk in chunks])
        self.terms = [own, place.swap(send, 8)]

    def far(self):
        high = self.place.at["z"] >> 1

        def sends(terms):
            total = terms[0] + terms[1]
            return pick(total, 0, high), pick(total, 0, 1 - high)

        own, send = self.place.chain.step(sends, self.terms)
        self.terms = [own, self.place.swap(send, 16)]

    def sum(self, terms):
        return terms[0] + terms[1]


PACK_FLIPS = ((0, 0), (0, 1), (1, 0), (1, 1))


def pack_kernel(orders, width, where, part, *outs):
    core = where[3]
    for i, order in enumerate(orders):
        cols = pl.ds(i * width, width)
        for j, (flip, flip_core) in enumerate(PACK_FLIPS):
            out = outs[4 * i + j]
            for k in (0, 1):
                if order[0] == "x":
                    out[k, 0] = part[0, k, where[2] ^ flip, core ^ flip_core, :, cols]
                else:
                    out[k, 0] = part[0, where[1] ^ flip, k, core ^ flip_core, :, cols]


def pack(place, where, part, rows, orders):
    total = part.shape[1]
    width = total // len(orders)
    part = part.reshape(4, 2, 2, 2, rows, total)
    n_out = 4 * len(orders)
    pieces = place.chain.step(lambda v: pl.pallas_call(
        functools.partial(pack_kernel, orders, width),
        grid_spec=pltpu.PrefetchScalarGridSpec(
            num_scalar_prefetch=1,
            grid=(4,),
            in_specs=[pl.BlockSpec((1, 2, 2, 2, rows, total), lambda z, where: (z, 0, 0, 0, 0, 0))],
            out_specs=[pl.BlockSpec((2, 1, rows, width), lambda z, where: (0, z, 0, 0))] * n_out,
        ),
        out_shape=[jax.ShapeDtypeStruct((2, 4, rows, width), BF16)] * n_out,
        cost_estimate=pl.CostEstimate(flops=10 ** 9, bytes_accessed=4 * 32 * rows * total, transcendentals=0),
        name="pack",
    )(*v), (where, part))
    chunks = []
    for i, order in enumerate(orders):
        chunk = Reduce(place, None, rows, order, (i * width, (i + 1) * width))
        chunk.packed = pieces[4 * i:4 * i + 4]
        chunks.append(chunk)
    return chunks


def send_first(chunks, hold=False):
    packed = [chunk.packed for chunk in chunks]
    if hold:
        packed = chunks[0].place.chain.step(lambda v: v, packed)
    for chunk, pieces in zip(chunks, packed):
        dim = chunk.order[0]
        chunk.terms = [pieces[0]] + [chunk.place.swap(piece, flip * MASKS[dim] + core) for (flip, core), piece in zip(PACK_FLIPS[1:], pieces[1:])]
        chunk.dims = [chunk.order[1], "z"]
        chunk.stage = 1


def join_kernel(last, where, own, far, own_core, far_core, *refs):
    out = refs[-1]
    core = where[3]
    bit = where[{"y": 1, "x": 2}[last]]
    for ref, flip, flip_core in ((own, 0, 0), (far, 1, 0), (own_core, 0, 1), (far_core, 1, 1)):
        for k in (0, 1):
            if last == "x":
                out[(where[0] & 1) ^ k, 0, bit ^ flip, core ^ flip_core] = ref[0, k]
            else:
                out[(where[0] & 1) ^ k, bit ^ flip, 0, core ^ flip_core] = ref[0, k]


def join(last, where, pieces, whole, cols, half):
    rows, part = pieces[0].shape[2:]

    def in_map(i, j, where):
        return (i, j, 0, 0)

    def out_map(i, j, where):
        if last == "x":
            return ((where[0] >> 1) ^ j, where[1] ^ i, 0, 0, 0, half)
        return ((where[0] >> 1) ^ j, 0, where[2] ^ i, 0, 0, half)

    block = (2, 1, 2, 2, rows, part) if last == "x" else (2, 2, 1, 2, rows, part)
    in_specs = [pl.BlockSpec((1, 2, rows, part), in_map)] * 4
    args = list(pieces)
    aliases = {}
    if whole is not None:
        in_specs = in_specs + [pl.BlockSpec(memory_space=pl.ANY)]
        args.append(whole)
        aliases = {5: 0}
    return pl.pallas_call(
        functools.partial(join_kernel, last),
        grid_spec=pltpu.PrefetchScalarGridSpec(num_scalar_prefetch=1, grid=(2, 2), in_specs=in_specs, out_specs=pl.BlockSpec(block, out_map)),
        out_shape=jax.ShapeDtypeStruct((4, 2, 2, 2, rows, cols), BF16),
        input_output_aliases=aliases,
        cost_estimate=pl.CostEstimate(flops=10 ** 9, bytes_accessed=8 * 8 * rows * part * 2, transcendentals=0),
    )(where, *args)


class Gather:
    def __init__(self, place, where, shard):
        self.place, self.where, self.cols = place, where, shard.shape[1]
        self.shard = shard
        self.second = ["y", "x"]
        self.third = ["x", "y"]

    def send_z(self):
        shard = self.place.chain.step(lambda shard: shard, self.shard)
        self.shards = [shard] + [self.place.swap(shard, 8 * flip) for flip in (1, 2, 3)]

    def send_second(self):
        half = self.cols // 2
        stacks = self.place.chain.step(lambda shards: [jnp.stack([shard[:, i * half:(i + 1) * half] for shard in shards]) for i in (0, 1)], self.shards)
        self.pieces = [[stack, self.place.swap(stack, MASKS[dim])] for stack, dim in zip(stacks, self.second)]

    def send_third(self):
        stacks = self.place.chain.step(lambda pieces: [jnp.stack(piece) for piece in pieces], self.pieces)
        self.pieces = [[stack, self.place.swap(stack, MASKS[dim]), self.place.swap(stack, 1)] for stack, dim in zip(stacks, self.third)]

    def send_core(self):
        far = self.place.chain.step(lambda value: value, [piece[1] for piece in self.pieces])
        self.pieces = [[piece[0], got, piece[2], self.place.swap(got, 1)] for piece, got in zip(self.pieces, far)]

    def whole(self):
        def both(pieces):
            left = join("x", self.where, pieces[0], None, self.cols, 0)
            return join("y", self.where, pieces[1], left, self.cols, 1).reshape(-1, self.cols)

        return self.place.chain.step(both, self.pieces)


def hidden_kernel(n_split, x_ref, g_ref, up_ref, down_ref, *refs):
    act_ref, pre_ref = refs[-2:]
    step = x_ref.shape[0] // n_split
    for i in range(n_split):
        rows = pl.ds(i * step, step)
        h = dot(x_ref[rows, :], up_ref[...], 1, 0)
        d_act = dot(g_ref[rows, :], down_ref[...], 1, 1)
        square = h * h
        t = jnp.tanh(GELU_SCALE * h * (1.0 + GELU_CUBIC * square))
        half = 0.5 * (1.0 + t)
        slope = half + 0.5 * h * (1.0 - t * t) * (GELU_SCALE * (1.0 + 3.0 * GELU_CUBIC * square))
        act_ref[rows, :] = (h * half).astype(BF16)
        pre_ref[rows, :] = (d_act * slope).astype(BF16)


def hidden_pair(layer, x_tokens, grad_cur, w_up, w_down, part=0, n_parts=1, slopes=None):
    _, tokens, width = x_tokens.shape
    ff_width = w_up.shape[2]
    tile = 512
    steps = ff_width // tile // n_parts
    base = part * steps
    kernel = functools.partial(hidden_kernel, 6)
    in_specs = [
        pl.BlockSpec((None, tokens, width), lambda j: (layer, 0, 0)),
        pl.BlockSpec((tokens, width), lambda j: (0, 0)),
        pl.BlockSpec((None, width, tile), lambda j: (layer, 0, base + j)),
        pl.BlockSpec((None, tile, width), lambda j: (layer, base + j, 0)),
    ]
    args = [x_tokens, grad_cur, w_up, w_down]
    aliases = {}
    if slopes is not None:
        in_specs.append(pl.BlockSpec(memory_space=pl.ANY))
        args.append(slopes)
        aliases = {4: 1}
    return pl.pallas_call(
        kernel,
        grid=(steps,),
        in_specs=in_specs,
        out_specs=[pl.BlockSpec((tokens, tile), lambda j: (0, j)), pl.BlockSpec((tokens, tile), lambda j: (0, base + j))],
        out_shape=(jax.ShapeDtypeStruct((tokens, ff_width // n_parts), BF16), jax.ShapeDtypeStruct((tokens, ff_width), BF16)),
        input_output_aliases=aliases,
        compiler_params=pltpu.CompilerParams(vmem_limit_bytes=56 * 2 ** 20),
        cost_estimate=pl.CostEstimate(flops=4 * tokens * width * ff_width // n_parts, bytes_accessed=70 * 10 ** 6 // n_parts, transcendentals=tokens * ff_width // n_parts),
    )(*args)


def act_kernel(n_split, x_ref, up_ref, *refs):
    act_ref = refs[-1]
    step = x_ref.shape[0] // n_split
    for i in range(n_split):
        rows = pl.ds(i * step, step)
        h = dot(x_ref[rows, :], up_ref[...], 1, 0)
        t = jnp.tanh(GELU_SCALE * h * (1.0 + GELU_CUBIC * (h * h)))
        act_ref[rows, :] = (h * (0.5 * (1.0 + t))).astype(BF16)


def hidden_act(x_in, w_up, part=0, n_parts=1, act=None):
    tokens, width = x_in.shape
    cols = w_up.shape[1]
    tile = 512
    steps = cols // tile
    in_specs = [pl.BlockSpec((tokens, width), lambda j: (0, 0)), pl.BlockSpec((width, tile), lambda j: (0, j))]
    args = [x_in, w_up]
    aliases = {}
    if act is not None:
        in_specs.append(pl.BlockSpec(memory_space=pl.ANY))
        args.append(act)
        aliases = {2: 0}
    return pl.pallas_call(
        functools.partial(act_kernel, 6),
        grid=(steps,),
        in_specs=in_specs,
        out_specs=pl.BlockSpec((tokens, tile), lambda j: (0, part * steps + j)),
        out_shape=jax.ShapeDtypeStruct((tokens, cols * n_parts), BF16),
        input_output_aliases=aliases,
        compiler_params=pltpu.CompilerParams(vmem_limit_bytes=48 * 2 ** 20),
        cost_estimate=pl.CostEstimate(flops=2 * tokens * width * cols, bytes_accessed=33 * 10 ** 6 // n_parts, transcendentals=tokens * cols),
    )(*args)


def total_square(value, place):
    value = value.reshape(1, 1)
    value = value + place.swap(value, 1) + place.swap(value, 2) + place.swap(value, 3)
    value = value + place.swap(value, 4) + place.swap(value, 8) + place.swap(value, 12)
    return (value + place.swap(value, 16))[0, 0]


def solution(mesh):
    n_dev = mesh.shape["fsdp"]
    rows_spec = P(None, "fsdp")

    def run(x_saved, grad_out, x_next, w_up, w_down, gacc_up, gacc_down, master_up, master_down, mom1_up, mom1_down, mom2_up, mom2_down):
        chain = Chain()
        place = Place(n_dev, chain)
        layers, model_width, ff_width = w_up.shape
        clip_norm = 0.1 * math.sqrt(2 * layers * model_width * ff_width)
        x_tokens = x_saved.reshape(layers, -1, model_width)
        grad_two = grad_out.reshape(-1, model_width)
        rows_up, rows_down = gacc_up.shape[1], gacc_down.shape[1]

        def weight_grad(pair):
            return dot(pair[0], pair[1], 0, 0).astype(BF16)

        where = jnp.stack([place.at[d] for d in "zyxc"]).astype(jnp.int32)

        def down_grad(act, grad):
            return chain.step(lambda v: weight_grad((v, grad)), act)

        def up_grad(layer, slopes):
            return chain.step(lambda v: weight_grad((x_tokens[layer], v)), slopes)

        act_low, slopes = chain.step(lambda v: hidden_pair(1, *v, part=0, n_parts=2), (x_tokens, grad_two, w_up, w_down))
        down_low = Reduce(place, down_grad(act_low, grad_two), rows_down, "xy", depth=2)
        down_low.first()
        act_high, pre_two = chain.step(lambda v: hidden_pair(1, *v[:4], part=1, n_parts=2, slopes=v[4]), (x_tokens, grad_two, w_up, w_down, slopes))
        down_high = Reduce(place, down_grad(act_high, grad_two), rows_down, "yx", depth=2)
        down_high.first()
        up_two = pack(place, where, up_grad(1, pre_two), rows_up, ("xyz", "yxz"))
        send_first(up_two)
        down_low.next()
        grad_one = chain.step(lambda v: (grad_two.astype(F32) + dot(v, w_up[1], 1, 1)).astype(BF16), pre_two)
        down_high.next()
        act_one, pre_one = chain.step(lambda v: hidden_pair(0, *v), (x_tokens, grad_one, w_up, w_down))
        for chunk in up_two:
            chunk.next()
        down_one = pack(place, where, down_grad(act_one, grad_one), rows_down, ("xyz", "yxz"))
        send_first(down_one)
        down_two = Merge(place, [down_low, down_high], True)
        up_one = pack(place, where, up_grad(0, pre_one), rows_up, ("xyz", "yxz", "xyz", "yxz"))
        send_first(up_one[:2])
        down_two.far()
        up_two = Merge(place, up_two)
        for chunk in down_one:
            chunk.next()
        up_two.far()
        up_one[0].next()
        up_one[1].next()
        send_first(up_one[2:], hold=True)
        down_one = Merge(place, down_one)
        up_one_left = Merge(place, up_one[:2])
        down_one.far()
        up_one_left.far()
        up_one[2].next()
        up_one[3].next()
        up_one_right = Merge(place, up_one[2:])

        def grads_of(chunks, gacc):
            def add(terms):
                sums = [chunk.sum(term) for chunk, term in zip(chunks, terms)]
                return (gacc + (sums[0] if len(sums) == 1 else jnp.concatenate(sums, axis=1))) / MICRO_STEPS

            return add

        def finish(chunks, gacc):
            return chain.step(grads_of(chunks, gacc), [chunk.terms for chunk in chunks])

        grad_down_two = finish([down_two], gacc_down[1])
        grad_up_two = finish([up_two], gacc_up[1])
        up_one_right.far()
        grad_down_one = finish([down_one], gacc_down[0])
        grad_up_one = finish([up_one_left, up_one_right], gacc_up[0])

        grads = (grad_up_one, grad_down_one, grad_up_two, grad_down_two)
        local_sq = chain.step(lambda v: sum(jnp.sum(g * g) for g in v), grads)
        clip_factor = jnp.minimum(1.0, clip_norm / jnp.sqrt(total_square(local_sq, place)))
        chain.last = None
        new_up = chain.step(lambda v: adamw_update(*v[:3], jnp.stack(v[3:5]) * v[5]), (master_up, mom1_up, mom2_up, grad_up_one, grad_up_two, clip_factor))
        up_shards = [new_up[0][i].astype(BF16) for i in (0, 1)]
        half_ff = ff_width // 2
        up_left, up_right = Gather(place, where, up_shards[0][:, :half_ff]), Gather(place, where, up_shards[0][:, half_ff:])
        up_b = Gather(place, where, up_shards[1])
        up_left.send_z()
        up_right.send_z()
        new_down = chain.step(lambda v: adamw_update(*v[:3], jnp.stack(v[3:5]) * v[5]), (master_down, mom1_down, mom2_down, grad_down_one, grad_down_two, clip_factor))
        down_a, down_b = [Gather(place, where, new_down[0][i].astype(BF16)) for i in (0, 1)]
        up_left.send_second()
        down_a.send_z()
        up_right.send_second()
        up_left.send_third()
        up_right.send_third()
        up_left.send_core()
        down_a.send_second()

        def down_mul(values):
            return (values[0].astype(F32) + dot(values[1], values[2], 1, 0)).astype(BF16)

        hidden_state = x_next.reshape(-1, model_width)
        weight = up_left.whole()
        down_a.send_third()
        up_b.send_z()
        act = chain.step(lambda v: hidden_act(*v, part=0, n_parts=2), (hidden_state, weight))
        up_right.send_core()
        weight = up_right.whole()
        down_a.send_core()
        up_b.send_second()
        act = chain.step(lambda v: hidden_act(*v[:2], part=1, n_parts=2, act=v[2]), (hidden_state, weight, act))
        down_b.send_z()
        up_b.send_third()
        hidden_state = chain.step(down_mul, (hidden_state, act, down_a.whole()))
        down_b.send_second()
        up_b.send_core()
        weight = up_b.whole()
        down_b.send_third()
        act = chain.step(lambda v: hidden_act(*v), (hidden_state, weight))
        down_b.send_core()
        hidden_state = chain.step(down_mul, (hidden_state, act, down_b.whole()))
        return (hidden_state.reshape(x_next.shape), new_up[0], new_down[0], new_up[1], new_down[1], new_up[2], new_down[2])

    return jax.shard_map(run, mesh=mesh, in_specs=(rows_spec, P("fsdp"), P("fsdp"), P(), P(), rows_spec, rows_spec, rows_spec, rows_spec, rows_spec, rows_spec, rows_spec, rows_spec), out_specs=(P("fsdp"), rows_spec, rows_spec, rows_spec, rows_spec, rows_spec, rows_spec), check_vma=False)
```
